32 devices in a mesh: dp: 8 (over z, y), shard: 4 (over x, core).
Axes of the slice: x: 2, y: 2, z: 4, core: 2. Of those that a mesh axis runs over, the one named last changes fastest.
Arguments:
- tokens: bfloat16 [512, 4096], P('shard', 'dp'), may hold values from -6 to 6
- cotangent: bfloat16 [512, 4096], P('shard', 'dp'), may hold values from -2 to 2
- expert_ids: int32 [512, 2], P('shard'), may hold values from 0 to 7, all different within a row; in each aligned block of 128 rows (0 to 127, 128 to 255, ...) at most 56 rows name the same one
- probs: float32 [512, 2], P('shard'), may hold values from 0.1 to 1
- gate_weight: bfloat16 [8, 4096, 768], P('shard', 'dp'), may hold values from -0.09375 to 0.09375
- up_weight: bfloat16 [8, 4096, 768], P('shard', 'dp'), may hold values from -0.09375 to 0.09375
- down_weight: bfloat16 [8, 768, 4096], P('shard', None, 'dp'), may hold values from -0.21875 to 0.21875
Outputs:
- mixed: bfloat16 [512, 4096], P('shard', 'dp')
- grad_tokens: bfloat16 [512, 4096], P('shard', 'dp')
- grad_gate: bfloat16 [8, 4096, 768], P('shard', 'dp')
- grad_up: bfloat16 [8, 4096, 768], P('shard', 'dp')
- grad_down: bfloat16 [8, 768, 4096], P('shard', None, 'dp')
The draws below stay inside these ranges and needn't reach their ends.
Inputs may be any that keep to these rules, and one draw needn't show every extreme that they name: `expert_ids`: each token names 2 different experts; among the 128 tokens of one index of shard no expert is named more than 56 times.
All inputs are finite; a program needn't handle non-finite values.
Results may differ from the reference program's by a relative error of at most 0.029.
Values may be sent and summed in bfloat16 or wider, within the bound.
No kernel may reach another device: no remote copies, remote signals or barrier semaphores. Data moves between devices by JAX's collectives and lax.ppermute only.
A program may use at most 64 MiB of HBM per device.

```python
import math
import jax
import jax.numpy as jnp
import numpy as np
from jax import lax

D = 4096
FF = 768
TOPW = 2
TOK_DEV = 128
EXPERTS = 8
TOKENS = 512
CAP = 56
N_DP = 8
N_SHARD = 4


def steps_of(rng, extent, shards, smallest, high):
    def one(axis_at, blocks):
        draws = jax.random.uniform(jax.random.fold_in(jax.random.fold_in(rng, 6), axis_at), (blocks,), jnp.float32, smallest / len(shards), high / len(shards))
        return jnp.repeat(jnp.exp(draws), extent[axis_at] // blocks).reshape((-1,) + (1,) * (len(extent) - axis_at - 1))

    loudness = one(*shards[0])
    for cut in shards[1:]:
        loudness = loudness * one(*cut)
    return loudness


def shared_out(rng, own, number, rows, amount, top, bound, lean):
    ranking = jax.random.permutation(rng, amount)
    packed, ordinary = portions_of(amount, rows * top, bound, lean, True), portions_of(amount, rows * top, bound, lean, False)
    places = jnp.arange(amount)

    def named(sizes, offset_by):
        used = int((sizes > 0).sum())
        fixed = max(1, used // 4)
        passed = fixed + (places - fixed + offset_by * (used - fixed)) % max(1, amount - fixed)
        return jnp.zeros((amount,), jnp.int32).at[ranking[jnp.where(places < fixed, places, passed)]].set(jnp.asarray(sizes, jnp.int32))

    sizes = jnp.where(number % 4 == 0, named(packed, number // 4), named(ordinary, number - number // 4 - 1))
    mixed = jax.random.permutation(jax.random.fold_in(own, 3), amount)
    donor, taker = mixed[0:amount // 2 * 2:2], mixed[1:amount // 2 * 2:2]
    room = jnp.minimum(sizes[donor] - 1, bound - sizes[taker]) // 2
    room = jnp.where((donor == ranking[0]) | (taker == ranking[0]) | (sizes[taker] == 0), 0, jnp.maximum(room, 0))
    passed = jax.random.randint(jax.random.fold_in(own, 4), (amount // 2,), 0, 1 << 20) % (room + 1)
    sizes = sizes.at[donor].add(-passed).at[taker].add(passed)
    labels = jnp.searchsorted(jnp.cumsum(sizes), jnp.arange(rows * top), side="right").astype(jnp.int32)
    table = labels.reshape(top, rows).T
    table = table[jax.random.permutation(jax.random.fold_in(own, 1), rows)]
    offset_by = jax.random.randint(jax.random.fold_in(own, 2), (rows, 1), 0, top)
    return jnp.take_along_axis(table, (jnp.arange(top)[None, :] + offset_by) % top, axis=1)


def portions_of(number_of, total, most, lean, full):
    weights = [(1 << 20) // math.isqrt(grade ** lean) + 1 for grade in range(1, number_of + 1)]
    largest = most if full else min(most, max(-(-total // number_of), total * weights[0] // sum(weights)))
    least = 1 if total - largest >= number_of - 1 else 0
    counts, spare = [largest] + [least] * (number_of - 1), total - largest - least * (number_of - 1)
    while spare > 0:
        candidates = [i for i in range(1, number_of) if counts[i] < largest] or [i for i in range(1, number_of) if counts[i] < most]
        pool, remaining = sum([weights[i] for i in candidates]), spare
        for i in candidates:
            more = min(most - counts[i], max(1, remaining * weights[i] // pool), spare)
            counts[i] = counts[i] + more
            spare = spare - more
    return np.array(counts)


def scatter_about(stream_key, shape, deviation, limit, shards=(), kind=jnp.bfloat16):
    drawn = deviation * jax.random.normal(stream_key, shape, jnp.float32)
    if shards:
        drawn = drawn * steps_of(stream_key, shape, shards, -0.22, 0.18)
    return jnp.clip(drawn, -limit, limit).astype(kind)


def setup_inputs(seed: int = 0) -> dict:
    splits = jax.random.split(jax.random.key(seed), 8)
    tokens = scatter_about(splits[0], (TOKENS, D), 1.0, 6.0, ((0, 4), (1, 8)))
    cotangent = scatter_about(splits[1], (TOKENS, D), 0.3, 2.0, ((0, 4), (1, 8)))
    expert_ids_keys = jax.random.split(jax.random.fold_in(splits[2], 1), TOKENS // TOK_DEV)
    expert_ids_turns = jax.random.permutation(jax.random.fold_in(splits[2], 3), TOKENS // TOK_DEV)
    expert_ids = jax.vmap(lambda own, number: shared_out(jax.random.fold_in(splits[2], 2), own, number, TOK_DEV, EXPERTS, TOPW, CAP, 2))(expert_ids_keys, expert_ids_turns).reshape((TOKENS, TOPW))
    probs = jnp.clip(0.1 + 0.9 * jax.random.uniform(splits[3], (TOKENS, TOPW), jnp.float32) ** steps_of(splits[3], (TOKENS, TOPW), ((0, 4),), -0.2, 0.2), 0.1, 1.0)
    gate_weight = scatter_about(splits[4], (EXPERTS, D, FF), D ** -0.5, 0.09375, ((0, 4), (1, 8)))
    up_weight = scatter_about(splits[5], (EXPERTS, D, FF), D ** -0.5, 0.09375, ((0, 4), (1, 8)))
    down_weight = scatter_about(splits[6], (EXPERTS, FF, D), FF ** -0.5, 0.21875, ((0, 4), (2, 8)))
    return {"tokens": tokens, "cotangent": cotangent, "expert_ids": expert_ids, "probs": probs, "gate_weight": gate_weight, "up_weight": up_weight, "down_weight": down_weight}


def block_sum(left, right_blocks, form):
    parts = jnp.einsum(form, left.astype(jnp.float32), right_blocks.astype(jnp.float32))
    parts = lax.optimization_barrier(parts.astype(jnp.bfloat16))
    return jnp.sum(parts.astype(jnp.float32), axis=1)


def reference(tokens, cotangent, expert_ids, probs, gate_weight, up_weight, down_weight):
    flat_ids = expert_ids.reshape(-1)
    flat_probs = probs.reshape(-1)
    most_rows = N_SHARD * CAP
    width = tokens.shape[1]
    block = width // N_DP
    units = gate_weight.shape[2]

    def one_expert(carry, expert):
        mixed_sum, grad_sum = carry
        found = flat_ids == expert
        pairs = jnp.nonzero(found, size=most_rows, fill_value=0)[0].astype(jnp.int32)
        valid = jnp.arange(most_rows) < jnp.sum(found.astype(jnp.int32))
        weight_row = jnp.where(valid, flat_probs[pairs], jnp.float32(0.0))
        token_row = (pairs // TOPW).astype(jnp.int32)
        rows_in = tokens[token_row]
        w_gate = gate_weight[expert]
        w_up = up_weight[expert]
        w_down = down_weight[expert]
        split_rows = rows_in.reshape(most_rows, N_DP, block)
        gate = block_sum(split_rows, w_gate.reshape(N_DP, block, units), "rsd,sdf->rsf")
        upward = block_sum(split_rows, w_up.reshape(N_DP, block, units), "rsd,sdf->rsf")
        sigmoid_gate = jax.nn.sigmoid(gate)
        activated = gate * sigmoid_gate
        hidden = (activated * upward).astype(jnp.bfloat16)
        expert_out = jnp.dot(hidden, w_down, preferred_element_type=jnp.float32).astype(jnp.bfloat16)
        mixed_sum = mixed_sum.at[token_row].add(weight_row[:, None] * expert_out.astype(jnp.float32))
        grad_out = (weight_row[:, None] * cotangent[token_row].astype(jnp.float32)).astype(jnp.bfloat16)
        grad_hidden = block_sum(grad_out.reshape(most_rows, N_DP, block),
                                w_down.reshape(units, N_DP, block), "rsd,fsd->rsf")
        grad_up_row = (grad_hidden * activated).astype(jnp.bfloat16)
        grad_gate_row = (grad_hidden * upward * sigmoid_gate * (1.0 + gate * (1.0 - sigmoid_gate))).astype(jnp.bfloat16)
        grad_down_w = jnp.dot(hidden.T, grad_out, preferred_element_type=jnp.float32).astype(jnp.bfloat16)
        grad_gate_w = jnp.dot(rows_in.T, grad_gate_row, preferred_element_type=jnp.float32).astype(jnp.bfloat16)
        grad_up_w = jnp.dot(rows_in.T, grad_up_row, preferred_element_type=jnp.float32).astype(jnp.bfloat16)
        grad_row = (jnp.dot(grad_gate_row, w_gate.T, preferred_element_type=jnp.float32)
                    + jnp.dot(grad_up_row, w_up.T, preferred_element_type=jnp.float32)).astype(jnp.bfloat16)
        grad_sum = grad_sum.at[token_row].add(grad_row.astype(jnp.float32))
        return (mixed_sum, grad_sum), (grad_gate_w, grad_up_w, grad_down_w)

    start = (jnp.zeros(tokens.shape, jnp.float32), jnp.zeros(tokens.shape, jnp.float32))
    (mixed_sum, grad_sum), (grad_gate, grad_up, grad_down) = lax.scan(
        one_expert, start, jnp.arange(EXPERTS, dtype=jnp.int32))
    return (mixed_sum.astype(jnp.bfloat16), grad_sum.astype(jnp.bfloat16), grad_gate, grad_up, grad_down)
```

```python
import jax
import jax.numpy as jnp
from jax import lax
from jax.sharding import PartitionSpec as P

BF = jnp.bfloat16
F32 = jnp.float32


def power_of_two(n):
    return n & (n - 1) == 0


def swap(x, axis, k):
    n = lax.axis_size(axis)
    return lax.ppermute(x, axis, [(i, i ^ k) for i in range(n)])


def gather_peers(x):
    n = lax.axis_size("shard")
    if power_of_two(n) and n <= 8:
        return [x] + [swap(x, "shard", k) for k in range(1, n)]
    every = lax.all_gather(x, "shard")
    return [every[k] for k in range(n)]


def peer_place(shard):
    n = lax.axis_size("shard")
    if power_of_two(n) and n <= 8:
        return shard ^ lax.axis_index("shard")
    return shard


def exchange_peers(blocks):
    n = lax.axis_size("shard")
    if power_of_two(n) and n <= 8:
        return [blocks[0]] + [swap(blocks[k], "shard", k) for k in range(1, n)]
    got = lax.all_to_all(jnp.stack(blocks), "shard", split_axis=0, concat_axis=0, tiled=True)
    return [got[k] for k in range(n)]


def sum_rows(x):
    n = lax.axis_size("dp")
    if not power_of_two(n):
        return lax.psum_scatter(x, "dp", scatter_dimension=0, tiled=True).astype(F32)
    me = lax.axis_index("dp")
    k = 1
    while k < n:
        half = x.shape[0] // 2
        bit = (me // k) % 2
        mine = lax.dynamic_slice_in_dim(x, bit * half, half, 0)
        other = lax.dynamic_slice_in_dim(x, (1 - bit) * half, half, 0)
        got = swap(other.astype(BF), "dp", k)
        x = mine.astype(F32) + got.astype(F32)
        k *= 2
    return x


def gather_rows(x):
    n = lax.axis_size("dp")
    if not power_of_two(n):
        return lax.all_gather(x, "dp", axis=0, tiled=True)
    me = lax.axis_index("dp")
    k = n // 2
    while k >= 1:
        got = swap(x, "dp", k)
        bit = (me // k) % 2
        x = jnp.where(bit == 1, jnp.concatenate((got, x)), jnp.concatenate((x, got)))
        k //= 2
    return x


def mm(form, a, b):
    return jnp.einsum(form, a, b, preferred_element_type=F32)


def local(tokens, cotangent, expert_ids, probs, gate_weight, up_weight, down_weight):
    token_count, slice_width = tokens.shape
    top = expert_ids.shape[1]
    held = gate_weight.shape[0]
    units = gate_weight.shape[2]
    shards = lax.axis_size("shard")
    experts = held * shards
    me = lax.axis_index("shard")
    capacity = 2 * max(1, 7 * token_count * top // (8 * experts))
    rows = shards * capacity

    meta = jnp.concatenate((expert_ids.T.astype(F32), probs.T), axis=0)
    metas = jnp.stack(gather_peers(meta))
    token_blocks = jnp.stack(gather_peers(tokens))
    cot_blocks = jnp.stack(gather_peers(cotangent))

    earlier = (
        jnp.arange(token_count)[:, None] < jnp.arange(token_count)[None, :]
    ).astype(BF)

    ids_in = metas[:, :top, :].astype(jnp.int32)
    probs_in = metas[:, top:, :]
    mine = (me * held + jnp.arange(held))[:, None, None, None]
    named = ids_in[None] == mine
    hit = jnp.any(named, axis=2)
    weight_of = jnp.sum(jnp.where(named, probs_in[None], 0.0), axis=2)
    place = mm("jst,tu->jsu", hit.astype(BF), earlier).astype(jnp.int32)
    slots = jnp.arange(capacity)[None, None, :, None]
    chosen = hit[:, :, None, :] & (place[:, :, None, :] == slots)
    pick = chosen.astype(BF)
    slot_prob = jnp.sum(jnp.where(chosen, weight_of[:, :, None, :], 0.0), axis=3)

    rows_in = mm("jsct,std->jscd", pick, token_blocks).astype(BF)
    rows_in = rows_in.reshape(held, rows, slice_width)
    gate_part = mm("jrd,jdf->jrf", rows_in, gate_weight).astype(BF)
    gate = sum_rows(gate_part.reshape(held * rows, units))
    up_part = mm("jrd,jdf->jrf", rows_in, up_weight).astype(BF)
    upward = sum_rows(up_part.reshape(held * rows, units))

    cot_rows = mm("jsct,std->jscd", pick, cot_blocks)
    grad_out = (slot_prob[..., None] * cot_rows).astype(BF).reshape(held, rows, slice_width)
    grad_part = mm("jrd,jfd->jrf", grad_out, down_weight).astype(BF)
    grad_hidden = sum_rows(grad_part.reshape(held * rows, units))

    sigmoid_gate = jax.nn.sigmoid(gate)
    activated = gate * sigmoid_gate
    hidden = gather_rows((activated * upward).astype(BF)).reshape(held, rows, units)
    grad_gate_row = (
        grad_hidden * upward * sigmoid_gate * (1.0 + gate * (1.0 - sigmoid_gate))
    ).astype(BF)
    grad_up_row = (grad_hidden * activated).astype(BF)
    gg = gather_rows(grad_gate_row).reshape(held, rows, units)
    gu = gather_rows(grad_up_row).reshape(held, rows, units)

    expert_out = mm("jrf,jfd->jrd", hidden, down_weight).astype(BF)
    expert_out = expert_out.reshape(held, shards, capacity, slice_width)
    returned = exchange_peers([expert_out[:, k] for k in range(shards)])
    grad_down = mm("jrf,jrd->jfd", hidden, grad_out).astype(BF)

    grad_row = (
        mm("jrf,jdf->jrd", gg, gate_weight) + mm("jrf,jdf->jrd", gu, up_weight)
    ).astype(BF)
    grad_row = grad_row.reshape(held, shards, capacity, slice_width)
    grad_back = exchange_peers([grad_row[:, k] for k in range(shards)])
    grad_gate = mm("jrd,jrf->jdf", rows_in, gg).astype(BF)
    grad_up = mm("jrd,jrf->jdf", rows_in, gu).astype(BF)

    home = expert_ids.T[None] == jnp.arange(experts)[:, None, None]
    home_hit = jnp.any(home, axis=1)
    home_place = mm("et,tu->eu", home_hit.astype(BF), earlier).astype(jnp.int32)
    spot = jnp.sum(jnp.where(home, home_place[:, None, :], 0), axis=0)
    owner = expert_ids.T // held
    slot = (peer_place(owner) * held + expert_ids.T % held) * capacity + spot
    back = (slot[:, :, None] == jnp.arange(experts * capacity)).astype(BF)
    out_rows = jnp.concatenate(returned).reshape(experts * capacity, slice_width)
    grad_rows = jnp.concatenate(grad_back).reshape(experts * capacity, slice_width)
    out_pairs = mm("ktr,rd->ktd", back, out_rows)
    mixed = jnp.sum(probs.T[:, :, None] * out_pairs, axis=0).astype(BF)
    grad_tokens = mm("tr,rd->td", jnp.sum(back, axis=0), grad_rows).astype(BF)
    return (mixed, grad_tokens, grad_gate, grad_up, grad_down)


def solution(mesh):
    placed = (
        P("shard", "dp"),
        P("shard", "dp"),
        P("shard", None),
        P("shard", None),
        P("shard", "dp", None),
        P("shard", "dp", None),
        P("shard", None, "dp"),
    )
    return jax.shard_map(
        local,
        mesh=mesh,
        in_specs=placed,
        out_specs=(
            P("shard", "dp"),
            P("shard", "dp"),
            P("shard", "dp", None),
            P("shard", "dp", None),
            P("shard", None, "dp"),
        ),
        check_vma=False,
    )
```

```python
import jax
import jax.numpy as jnp
from jax import lax
from jax.sharding import PartitionSpec as P


BF = jnp.bfloat16
F32 = jnp.float32
CUTS = 2
CROSS = ((0,1), (1,0), (0,1), (0,1), (1,0), (0,1))


def power_of_two(n):
    return n & (n - 1) == 0


def swap(x, axis, k):
    n = lax.axis_size(axis)
    return lax.ppermute(x, axis, [(i, i ^ k) for i in range(n)])


def gather_peers(x, after=None):
    n = lax.axis_size("shard")
    if not (power_of_two(n) and n <= 8):
        every = lax.all_gather(x, "shard")
        return [every[k] for k in range(n)]
    blocks = [x]
    k = n // 2
    while k >= 1:
        sent = blocks
        if after is not None and k == n // 2:
            sent = [lax.optimization_barrier((x, after))[0]]
        got = []
        for block in sent:
            got.append(swap(block, "shard", k))
        blocks = [b for pair in zip(blocks, got) for b in pair]
        k //= 2
    return blocks


def peer_place(shard):
    n = lax.axis_size("shard")
    if power_of_two(n) and n <= 8:
        return shard ^ lax.axis_index("shard")
    return shard


def exchange_peers(blocks):
    n = lax.axis_size("shard")
    if power_of_two(n) and n <= 8:
        return [blocks[0]] + [swap(blocks[k], "shard", k) for k in range(1, n)]
    got = lax.all_to_all(jnp.stack(blocks), "shard", split_axis=0, concat_axis=0, tiled=True)
    return [got[k] for k in range(n)]


def halvings(crossed):
    n = lax.axis_size("dp")
    order = []
    while 1 << (len(order) + 1) < n:
        order.append((1 << len(order), len(order)))
    if crossed and len(order) > 1:
        order[0], order[1] = order[1], order[0]
    return order


def bit_of(k):
    return (lax.axis_index("dp") // k) % 2


def sum_rows(x, crossed=False):
    n = lax.axis_size("dp")
    if not power_of_two(n):
        return lax.psum_scatter(x, "dp", scatter_dimension=0, tiled=True).astype(F32)
    order = halvings(crossed)
    x = x.reshape((2,) * len(order) + (-1, x.shape[-1]))
    gone = []
    for k, place in order:
        axis = place - sum(g < place for g in gone)
        gone.append(place)
        bit = bit_of(k)
        mine = lax.dynamic_index_in_dim(x, bit, axis, keepdims=False)
        other = lax.dynamic_index_in_dim(x, 1 - bit, axis, keepdims=False)
        got = swap(other.astype(BF), "dp", k)
        x = mine.astype(F32) + got.astype(F32)
    if n > 1:
        x = x.astype(BF)
        x = x.astype(F32) + swap(x, "dp", n // 2).astype(F32)
    return x


def gather_rows(x, crossed=False):
    n = lax.axis_size("dp")
    if not power_of_two(n):
        return lax.all_gather(x, "dp", axis=0, tiled=True)
    units = x.shape[-1]
    here = []
    for k, place in reversed(halvings(crossed)):
        axis = sum(h < place for h in here)
        here.append(place)
        got = swap(x, "dp", k)
        x = jnp.where(bit_of(k) == 1, jnp.stack((got, x), axis), jnp.stack((x, got), axis))
    return x.reshape(-1, units)


def mm(form, a, b):
    return jnp.einsum(form, a, b, preferred_element_type=F32)


def local(tokens, cotangent, expert_ids, probs, gate_weight, up_weight, down_weight):
    token_count, slice_width = tokens.shape
    top = expert_ids.shape[1]
    held = gate_weight.shape[0]
    units = gate_weight.shape[2]
    shards = lax.axis_size("shard")
    experts = held * shards
    me = lax.axis_index("shard")
    capacity = 2 * max(1, 7 * token_count * top // (8 * experts))
    rows = shards * capacity

    meta = jnp.concatenate((expert_ids.T.astype(F32), probs.T), axis=0)
    token_blocks = gather_peers(tokens)
    metas = jnp.stack(gather_peers(meta))
    cot_blocks = gather_peers(cotangent, token_blocks[shards // 2])

    earlier = (
        jnp.arange(token_count)[:, None] < jnp.arange(token_count)[None, :]
    ).astype(BF)

    ids_in = metas[:, :top, :].astype(jnp.int32)
    probs_in = metas[:, top:, :]
    mine = (me * held + jnp.arange(held))[:, None, None, None]
    named = ids_in[None] == mine
    hit = jnp.any(named, axis=2)
    weight_of = jnp.sum(jnp.where(named, probs_in[None], 0.0), axis=2)
    place = mm("jst,tu->jsu", hit.astype(BF), earlier).astype(jnp.int32)
    slots = jnp.arange(capacity)[None, None, :, None]
    chosen = hit[:, :, None, :] & (place[:, :, None, :] == slots)
    pick = chosen.astype(BF)
    slot_prob = jnp.sum(jnp.where(chosen, weight_of[:, :, None, :], 0.0), axis=3)

    rows_in = jnp.stack(
        [mm("jct,td->jcd", pick[:, k], token_blocks[k]).astype(BF) for k in range(shards)], axis=1
    )
    grad_out = jnp.stack(
        [
            (slot_prob[:, k, :, None] * mm("jct,td->jcd", pick[:, k], cot_blocks[k])).astype(BF)
            for k in range(shards)
        ],
        axis=1,
    ).reshape(held, rows, slice_width)
    rows_in = rows_in.reshape(held, rows, slice_width)
    gate_part = mm("jrd,jdf->jrf", rows_in, gate_weight).astype(BF).reshape(held * rows, units)
    up_part = mm("jrd,jdf->jrf", rows_in, up_weight).astype(BF).reshape(held * rows, units)
    grad_part = mm("jrd,jfd->jrf", grad_out, down_weight).astype(BF).reshape(held * rows, units)

    cuts = CUTS if units % (128 * CUTS) == 0 else 1
    wide = units // cuts
    hidden, gg, gu = [], [], []
    for cut in range(cuts):
        part = slice(cut * wide, (cut + 1) * wide)
        gate = sum_rows(gate_part[:, part], CROSS[0][cut])
        upward = sum_rows(up_part[:, part], CROSS[1][cut])
        grad_hidden = sum_rows(grad_part[:, part], CROSS[2][cut])
        sigmoid_gate = jax.nn.sigmoid(gate)
        activated = gate * sigmoid_gate
        hidden.append(gather_rows((activated * upward).astype(BF), CROSS[3][cut]))
        grad_gate_row = (
            grad_hidden * upward * sigmoid_gate * (1.0 + gate * (1.0 - sigmoid_gate))
        ).astype(BF)
        grad_up_row = (grad_hidden * activated).astype(BF)
        gg.append(gather_rows(grad_gate_row, CROSS[4][cut]))
        gu.append(gather_rows(grad_up_row, CROSS[5][cut]))
    hidden, gg, gu = (
        jnp.concatenate(x, axis=1).reshape(held, rows, units) for x in (hidden, gg, gu)
    )

    expert_out = mm("jrf,jfd->jrd", hidden, down_weight).astype(BF)
    expert_out = expert_out.reshape(held, shards, capacity, slice_width)
    returned = exchange_peers([expert_out[:, k] for k in range(shards)])
    grad_down = mm("jrf,jrd->jfd", hidden, grad_out).astype(BF)

    grad_row = (
        mm("jrf,jdf->jrd", gg, gate_weight) + mm("jrf,jdf->jrd", gu, up_weight)
    ).astype(BF)
    gg, gu, grad_row = lax.optimization_barrier((gg, gu, grad_row))
    grad_row = grad_row.reshape(held, shards, capacity, slice_width)
    grad_back = exchange_peers([grad_row[:, k] for k in range(shards)])
    grad_gate = mm("jrd,jrf->jdf", rows_in, gg).astype(BF)
    grad_up = mm("jrd,jrf->jdf", rows_in, gu).astype(BF)

    home = expert_ids.T[None] == jnp.arange(experts)[:, None, None]
    home_hit = jnp.any(home, axis=1)
    home_place = mm("et,tu->eu", home_hit.astype(BF), earlier).astype(jnp.int32)
    spot = jnp.sum(jnp.where(home, home_place[:, None, :], 0), axis=0)
    owner = expert_ids.T // held
    slot = (peer_place(owner) * held + expert_ids.T % held) * capacity + spot
    back = (slot[:, :, None] == jnp.arange(experts * capacity)).astype(BF)
    out_rows = jnp.concatenate(returned).reshape(experts * capacity, slice_width)
    grad_rows = jnp.concatenate(grad_back).reshape(experts * capacity, slice_width)
    out_pairs = mm("ktr,rd->ktd", back, out_rows)
    mixed = jnp.sum(probs.T[:, :, None] * out_pairs, axis=0).astype(BF)
    grad_tokens = mm("tr,rd->td", jnp.sum(back, axis=0), grad_rows).astype(BF)
    return (mixed, grad_tokens, grad_gate, grad_up, grad_down)


def solution(mesh):
    placed = (
        P("shard", "dp"),
        P("shard", "dp"),
        P("shard", None),
        P("shard", None),
        P("shard", "dp", None),
        P("shard", "dp", None),
        P("shard", None, "dp"),
    )
    return jax.shard_map(
        local,
        mesh=mesh,
        in_specs=placed,
        out_specs=(
            P("shard", "dp"),
            P("shard", "dp"),
            P("shard", "dp", None),
            P("shard", "dp", None),
            P("shard", None, "dp"),
        ),
        check_vma=False,
    )
```

```python
import jax
import jax.numpy as jnp
from jax import lax
from jax.sharding import PartitionSpec as P


BF = jnp.bfloat16
F32 = jnp.float32
CUTS = 2
CROSS = ((0,1), (1,0), (0,1), (0,1), (1,0), (0,1))


def power_of_two(n):
    return n & (n - 1) == 0


def swap(x, axis, k):
    n = lax.axis_size(axis)
    return lax.ppermute(x, axis, [(i, i ^ k) for i in range(n)])


def gather_peers(x, after=None):
    n = lax.axis_size("shard")
    if not (power_of_two(n) and n <= 8):
        every = lax.all_gather(x, "shard")
        return [every[k] for k in range(n)]
    blocks = [x]
    k = n // 2
    while k >= 1:
        sent = blocks
        if after is not None and k == n // 2:
            sent = [lax.optimization_barrier((x, after))[0]]
        got = []
        for block in sent:
            got.append(swap(block, "shard", k))
        blocks = [b for pair in zip(blocks, got) for b in pair]
        k //= 2
    return blocks


def peer_place(shard):
    n = lax.axis_size("shard")
    if power_of_two(n) and n <= 8:
        return shard ^ lax.axis_index("shard")
    return shard


def exchange_peers(blocks):
    n = lax.axis_size("shard")
    if power_of_two(n) and n <= 8:
        return [blocks[0]] + [swap(blocks[k], "shard", k) for k in range(1, n)]
    got = lax.all_to_all(jnp.stack(blocks), "shard", split_axis=0, concat_axis=0, tiled=True)
    return [got[k] for k in range(n)]


def halvings(crossed):
    n = lax.axis_size("dp")
    order = []
    while 1 << (len(order) + 1) < n:
        order.append((1 << len(order), len(order)))
    if crossed and len(order) > 1:
        order[0], order[1] = order[1], order[0]
    return order


def bit_of(k):
    return (lax.axis_index("dp") // k) % 2


def sum_rows(x, crossed):
    n = lax.axis_size("dp")
    if not power_of_two(n):
        return lax.psum_scatter(x, "dp", scatter_dimension=0, tiled=True).astype(F32)
    order = halvings(crossed)
    x = x.reshape((2,) * len(order) + (-1, x.shape[-1]))
    gone = []
    for k, place in order:
        axis = place - sum(g < place for g in gone)
        gone.append(place)
        bit = bit_of(k)
        mine = lax.dynamic_index_in_dim(x, bit, axis, keepdims=False)
        other = lax.dynamic_index_in_dim(x, 1 - bit, axis, keepdims=False)
        got = swap(other.astype(BF), "dp", k)
        x = mine.astype(F32) + got.astype(F32)
    if n > 1:
        x = x.astype(BF)
        got = swap(x, "dp", n // 2)
        x = x.astype(F32) + got.astype(F32)
    return x


def gather_rows(x, crossed):
    n = lax.axis_size("dp")
    if not power_of_two(n):
        return lax.all_gather(x, "dp", axis=0, tiled=True)
    units = x.shape[-1]
    here = []
    for k, place in reversed(halvings(crossed)):
        axis = sum(h < place for h in here)
        here.append(place)
        got = swap(x, "dp", k)
        x = jnp.where(bit_of(k) == 1, jnp.stack((got, x), axis), jnp.stack((x, got), axis))
    return x.reshape(-1, units)


def mm(form, a, b):
    return jnp.einsum(form, a, b, preferred_element_type=F32)


def local(tokens, cotangent, expert_ids, probs, gate_weight, up_weight, down_weight):
    token_count, slice_width = tokens.shape
    top = expert_ids.shape[1]
    held = gate_weight.shape[0]
    units = gate_weight.shape[2]
    shards = lax.axis_size("shard")
    experts = held * shards
    me = lax.axis_index("shard")
    capacity = 2 * max(1, 7 * token_count * top // (8 * experts))
    rows = shards * capacity

    meta = jnp.concatenate((expert_ids.T.astype(F32), probs.T), axis=0)
    token_blocks = gather_peers(tokens)
    metas = gather_peers(meta)
    cot_blocks = gather_peers(cotangent, token_blocks[shards // 2])

    earlier = (
        jnp.arange(token_count)[:, None] < jnp.arange(token_count)[None, :]
    ).astype(BF)

    def picks(metas):
        ids_in = metas[:, :top, :].astype(jnp.int32)
        probs_in = metas[:, top:, :]
        mine = (me * held + jnp.arange(held))[:, None, None, None]
        named = ids_in[None] == mine
        hit = jnp.any(named, axis=2)
        weight_of = jnp.sum(jnp.where(named, probs_in[None], 0.0), axis=2)
        place = mm("jst,tu->jsu", hit.astype(BF), earlier).astype(jnp.int32)
        slots = jnp.arange(capacity)[None, None, :, None]
        chosen = hit[:, :, None, :] & (place[:, :, None, :] == slots)
        slot_prob = jnp.sum(jnp.where(chosen, weight_of[:, :, None, :], 0.0), axis=3)
        return chosen.astype(BF), slot_prob

    pick, slot_prob = picks(jnp.stack(metas))

    rows_in = jnp.stack(
        [mm("jct,td->jcd", pick[:, k], token_blocks[k]).astype(BF) for k in range(shards)], axis=1
    )
    rows_in = rows_in.reshape(held, rows, slice_width)
    gate_part = mm("jrd,jdf->jrf", rows_in, gate_weight).astype(BF).reshape(held * rows, units)
    up_part = mm("jrd,jdf->jrf", rows_in, up_weight).astype(BF).reshape(held * rows, units)
    up_part, pick = lax.optimization_barrier((up_part, pick))
    grad_out = jnp.stack(
        [
            (slot_prob[:, k, :, None] * mm("jct,td->jcd", pick[:, k], cot_blocks[k])).astype(BF)
            for k in range(shards)
        ],
        axis=1,
    ).reshape(held, rows, slice_width)
    grad_part = mm("jrd,jfd->jrf", grad_out, down_weight).astype(BF).reshape(held * rows, units)

    cuts = CUTS if units % (128 * CUTS) == 0 else 1
    wide = units // cuts
    hidden, gg, gu = [], [], []
    for cut in range(cuts):
        part = slice(cut * wide, (cut + 1) * wide)
        gate = sum_rows(gate_part[:, part], CROSS[0][cut])
        upward = sum_rows(up_part[:, part], CROSS[1][cut])
        grad_hidden = sum_rows(grad_part[:, part], CROSS[2][cut])
        sigmoid_gate = jax.nn.sigmoid(gate)
        activated = gate * sigmoid_gate
        hidden.append(gather_rows((activated * upward).astype(BF), CROSS[3][cut]))
        grad_gate_row = (
            grad_hidden * upward * sigmoid_gate * (1.0 + gate * (1.0 - sigmoid_gate))
        ).astype(BF)
        grad_up_row = (grad_hidden * activated).astype(BF)
        gg.append(gather_rows(grad_gate_row, CROSS[4][cut]))
        gu.append(gather_rows(grad_up_row, CROSS[5][cut]))
    hidden, gg, gu = (
        jnp.concatenate(x, axis=1).reshape(held, rows, units) for x in (hidden, gg, gu)
    )

    expert_out = mm("jrf,jfd->jrd", hidden, down_weight).astype(BF)
    expert_out = expert_out.reshape(held, shards, capacity, slice_width)
    returned = exchange_peers([expert_out[:, k] for k in range(shards)])
    grad_row = (
        mm("jrf,jdf->jrd", gg, gate_weight) + mm("jrf,jdf->jrd", gu, up_weight)
    ).astype(BF)
    hidden, gg, gu, grad_row = lax.optimization_barrier((hidden, gg, gu, grad_row))
    grad_row = grad_row.reshape(held, shards, capacity, slice_width)
    grad_back = exchange_peers([grad_row[:, k] for k in range(shards)])
    grad_down = mm("jrf,jrd->jfd", hidden, grad_out).astype(BF)
    grad_gate = mm("jrd,jrf->jdf", rows_in, gg).astype(BF)
    grad_up = mm("jrd,jrf->jdf", rows_in, gu).astype(BF)

    home = expert_ids.T[None] == jnp.arange(experts)[:, None, None]
    home_hit = jnp.any(home, axis=1)
    home_place = mm("et,tu->eu", home_hit.astype(BF), earlier).astype(jnp.int32)
    spot = jnp.sum(jnp.where(home, home_place[:, None, :], 0), axis=0)
    owner = expert_ids.T // held
    slot = (peer_place(owner) * held + expert_ids.T % held) * capacity + spot
    back = (slot[:, :, None] == jnp.arange(experts * capacity)).astype(BF)
    out_rows = jnp.concatenate(returned).reshape(experts * capacity, slice_width)
    grad_rows = jnp.concatenate(grad_back).reshape(experts * capacity, slice_width)
    out_pairs = mm("ktr,rd->ktd", back, out_rows)
    mixed = jnp.sum(probs.T[:, :, None] * out_pairs, axis=0).astype(BF)
    either = lax.optimization_barrier(jnp.sum(back, axis=0))
    grad_tokens = mm("tr,rd->td", either, grad_rows).astype(BF)
    return (mixed, grad_tokens, grad_gate, grad_up, grad_down)


def solution(mesh):
    placed = (
        P("shard", "dp"),
        P("shard", "dp"),
        P("shard", None),
        P("shard", None),
        P("shard", "dp", None),
        P("shard", "dp", None),
        P("shard", None, "dp"),
    )
    return jax.shard_map(
        local,
        mesh=mesh,
        in_specs=placed,
        out_specs=(
            P("shard", "dp"),
            P("shard", "dp"),
            P("shard", "dp", None),
            P("shard", "dp", None),
            P("shard", None, "dp"),
        ),
        check_vma=False,
    )
```
